32 devices in a mesh: inst: 4 (over x, core), dp: 4 (over z), tp: 2 (over y).
Axes of the slice: x: 2, y: 2, z: 4, core: 2. Of those that a mesh axis runs over, the one named last changes fastest.
Arguments:
- kernel_grads: bfloat16 [16, 2, 128, 4608], P(('inst', 'dp'), 'tp'), may hold values from -0.75 to 0.75
- kernel_master: float32 [2, 128, 4608], P('tp', 'dp'), may hold values from -6 to 6
- kernel_first: float32 [2, 128, 4608], P('tp', 'dp'), may hold values from -3 to 3
- kernel_second: float32 [2, 128, 4608], P('tp', 'dp'), may hold values from 0.05 to 4
- gain_grads: bfloat16 [32, 4, 4608], P(('inst', 'dp', 'tp')), may hold values from -0.29882812 to 0.29882812
- gain_master: float32 [4, 4608], replicated, may hold values from -6 to 6
- gain_first: float32 [4, 4608], replicated, may hold values from -3 to 3
- gain_second: float32 [4, 4608], replicated, may hold values from 0.05 to 4
Outputs:
- kernel_params: bfloat16 [2, 128, 4608], P('tp')
- kernel_master_new: float32 [2, 128, 4608], P('tp', 'dp')
- kernel_first_new: float32 [2, 128, 4608], P('tp', 'dp')
- kernel_second_new: float32 [2, 128, 4608], P('tp', 'dp')
- gain_params: bfloat16 [4, 4608], replicated
- gain_master_new: float32 [4, 4608], replicated
- gain_first_new: float32 [4, 4608], replicated
- gain_second_new: float32 [4, 4608], replicated
The draws below stay inside these ranges and needn't reach their ends.
All inputs are finite; a program needn't handle non-finite values.
Results may differ from the reference program's by a relative error of at most 0.004.
Values may be sent and summed in bfloat16 or wider, within the bound.
A program may use at most 64 MiB of HBM per device.

```python
import math
import jax
import jax.numpy as jnp
from jax import lax

D = 4608
HEAD_DIM = 128
NORMS = 4
KVH = 2
REPLICAS = 16
DEVICES = 32


def spiked(array, rng, source, target, blocks, factor):
    owner, partner = [(jnp.arange(array.shape[dim]) // (array.shape[dim] // blocks)).reshape([-1 if axis == dim else 1 for axis in range(array.ndim)]) for dim in (source, target)]
    chosen = jax.random.permutation(rng, blocks)[partner]
    strong = (owner == chosen) | (owner == (partner + blocks // 2) % blocks)
    return jnp.where(strong, factor * array, array)


def block_levels(rng, extent, split, least, largest):
    level, own = 1.0, jax.random.fold_in(rng, 6)
    for axis_at, shards_of in split:
        steps = jnp.exp(jax.random.uniform(jax.random.fold_in(own, axis_at), (shards_of,), jnp.float32, least / len(split), largest / len(split)))
        level = level * jnp.repeat(steps, extent[axis_at] // shards_of).reshape([-1 if axis == axis_at else 1 for axis in range(len(extent))])
    return level


def normal_values(key, dims, spread, most, split=(), dtype=jnp.bfloat16):
    drawn = jax.random.normal(key, dims, jnp.float32) * spread
    if len(split) > 0:
        drawn = block_levels(key, dims, split, -0.22, 0.18) * drawn
    return jnp.clip(drawn, min=-most, max=most).astype(dtype)


def bell_draw_with(rng, dims, spread, reach, shards, heavy, kind=jnp.bfloat16):
    result = spread * jax.random.normal(rng, dims, jnp.float32)
    if shards:
        result = result * block_levels(rng, dims, shards, -0.22, 0.18)
    return jnp.clip(spiked(result, jax.random.fold_in(rng, 3), *heavy), -reach, reach).astype(kind)


def setup_inputs(seed: int = 0) -> dict:
    arg_keys = jax.random.split(jax.random.key(seed), 9)
    return {
        "kernel_grads": bell_draw_with(arg_keys[0], (REPLICAS, KVH, HEAD_DIM, D), 0.125, 0.75, ((0, 16), (1, 2)), (0, 2, 16, 2.0)),
        "kernel_master": normal_values(arg_keys[1], (KVH, HEAD_DIM, D), 1.0, 6.0, ((0, 2), (1, 4)), jnp.float32),
        "kernel_first": normal_values(arg_keys[2], (KVH, HEAD_DIM, D), 0.5, 3.0, ((0, 2), (1, 4)), jnp.float32),
        "kernel_second": jnp.clip(jnp.exp(math.log(4.0) - 4.3820266 * jax.random.uniform(arg_keys[3], (KVH, HEAD_DIM, D), jnp.float32) ** block_levels(arg_keys[3], (KVH, HEAD_DIM, D), ((0, 2), (1, 4)), -0.2, 0.2)), 0.05, 4.0),
        "gain_grads": bell_draw_with(arg_keys[4], (DEVICES, NORMS, D), 0.05, 0.29882812, ((0, 32),), (0, 2, 32, 2.75)),
        "gain_master": normal_values(arg_keys[5], (NORMS, D), 1.0, 6.0, (), jnp.float32),
        "gain_first": normal_values(arg_keys[6], (NORMS, D), 0.5, 3.0, (), jnp.float32),
        "gain_second": jnp.clip(jnp.exp(jax.random.uniform(arg_keys[7], (NORMS, D), jnp.float32, math.log(0.05), math.log(4.0))), 0.05, 4.0),
    }


beta_one = 0.9
beta_two = 0.95
learn_rate = 0.01
decay_rate = 0.1
epsilon = 1e-08
step_count = 100.0

def adam_update(gradient, master, first_moment, second_moment):
    first_next = beta_one * first_moment + (1.0 - beta_one) * gradient
    second_next = beta_two * second_moment + (1.0 - beta_two) * gradient * gradient
    first_hat = first_next / (1.0 - beta_one ** step_count)
    second_hat = second_next / (1.0 - beta_two ** step_count)
    master_next = master - learn_rate * (first_hat / (jnp.sqrt(second_hat) + epsilon) + decay_rate * master)
    return (master_next, first_next, second_next)

def reference(kernel_grads, kernel_master, kernel_first, kernel_second, gain_grads, gain_master, gain_first, gain_second):

    def accumulate(running, portion):
        return (running + portion.astype(jnp.float32), None)
    kernel_sum, unused = lax.scan(accumulate, jnp.zeros(kernel_grads.shape[1:], jnp.float32), kernel_grads)
    gain_sum, unused_gain = lax.scan(accumulate, jnp.zeros(gain_grads.shape[1:], jnp.float32), gain_grads)
    kernel_master_new, kernel_first_new, kernel_second_new = adam_update(kernel_sum, kernel_master, kernel_first, kernel_second)
    gain_master_new, gain_first_new, gain_second_new = adam_update(gain_sum, gain_master, gain_first, gain_second)
    kernel_params = kernel_master_new.astype(jnp.bfloat16)
    gain_params = gain_master_new.astype(jnp.bfloat16)
    return (kernel_params, kernel_master_new, kernel_first_new, kernel_second_new, gain_params, gain_master_new, gain_first_new, gain_second_new)
```

```python
import functools

import jax
import jax.numpy as jnp
from jax import lax
from jax.experimental import pallas as pl
from jax.experimental.pallas import tpu as pltpu
from jax.sharding import PartitionSpec as P

beta_one = 0.9
beta_two = 0.95
learn_rate = 0.01
decay_rate = 0.1
epsilon = 1e-08
step_count = 100.0
MESH = pl.DeviceIdType.MESH
F32 = jnp.float32
BF16 = jnp.bfloat16


def adam_update(gradient, master, first_moment, second_moment):
    first_next = beta_one * first_moment + (1.0 - beta_one) * gradient
    second_next = beta_two * second_moment + (1.0 - beta_two) * gradient * gradient
    first_hat = first_next / (1.0 - beta_one**step_count)
    second_hat = second_next / (1.0 - beta_two**step_count)
    master_next = master - learn_rate * (
        first_hat / (jnp.sqrt(second_hat) + epsilon) + decay_rate * master
    )
    return (master_next, first_next, second_next)


def step_kernel(
    n, tp, grads, master, first, second, gains,
    params, gsum, gain_sum,
    gv, core_in, x_out, x_in, z_out, z_in, pv, mv, vv,
    nv, nc_in, nx_out, nx_in, ny, nz,
    load_sem, core_s, core_r, x_s, x_r, z_s, z_r,
    pz_s, pz_r, px_s, px_r, pc_s, pc_r, g_s, g_r,
    nc_s, nc_r, nx_s, nx_r, ny_s, ny_r, nz_s, nz_r, nf_s, nf_r,
):
    cols = gv.shape[2]
    half, quarter = cols // 2, cols // 4
    me = lax.axis_index("inst")
    z = lax.axis_index("dp")
    y = lax.axis_index("tp")
    core, x = me % 2, me // 2
    partner = me + 1 - 2 * core
    across = (me + 2) % 4
    diagonal = (partner + 2) % 4
    order = sorted(range(1, n), key=lambda j: -min(j, n - j)) + [0]
    near = sorted(range(1, n), key=lambda j: min(j, n - j))

    def span(start, size):
        return pl.ds(pl.multiple_of(start, 128), size)

    def cols_of(inst):
        return span((inst % 2) * half + (inst // 2) * quarter, quarter)

    def send(src, dst, s, r, **where):
        copy = pltpu.make_async_remote_copy(
            src_ref=src, dst_ref=dst, send_sem=s, recv_sem=r,
            device_id=where, device_id_type=MESH,
        )
        copy.start()
        return copy

    def load(src, dst, k):
        copy = pltpu.make_async_copy(src, dst, load_sem.at[k])
        copy.start()
        return copy

    to = {j: (z + j) % n for j in range(n)}
    frm = {j: (z + n - j) % n for j in range(n)}
    loads = {j: load(grads.at[to[j]], gv.at[to[j]], j) for j in order}
    load_gain = load(gains, nv, n)
    load_state = [
        load(a, b, n + 1 + k)
        for k, (a, b) in enumerate(((master, pv), (first, mv), (second, vv)))
    ]

    barrier = pltpu.get_barrier_semaphore()
    for other in (partner, across, diagonal):
        pl.semaphore_signal(barrier, inc=1, device_id={"inst": other}, device_id_type=MESH)
    for j in range(1, n):
        pl.semaphore_signal(barrier, inc=1, device_id={"dp": to[j]}, device_id_type=MESH)
    for j in range(1, tp):
        pl.semaphore_signal(
            barrier, inc=1, device_id={"tp": (y + j) % tp}, device_id_type=MESH
        )
    pl.semaphore_wait(barrier, 3 + n - 1 + tp - 1)

    mine_half, other_half = span(core * half, half), span((1 - core) * half, half)
    mine, theirs = cols_of(me), cols_of(across)
    mine_in, theirs_in = span(x * quarter, quarter), span((1 - x) * quarter, quarter)
    sent = []

    core_c = {}
    for j in order:
        loads[j].wait()
        core_c[j] = send(
            gv.at[to[j], :, other_half], core_in.at[to[j]], core_s.at[j], core_r.at[j],
            inst=partner,
        )
    load_gain.wait()
    nc = send(nv.at[:, other_half], nc_in, nc_s.at[0], nc_r.at[0], inst=partner)

    x_c = {}
    for j in order:
        core_c[j].wait_recv()
        k = to[j]
        x_out[k] = (
            gv[k, :, theirs].astype(F32) + core_in[k, :, theirs_in].astype(F32)
        ).astype(BF16)
        x_c[j] = send(x_out.at[k], x_in.at[k], x_s.at[j], x_r.at[j], inst=across)
        if j == order[0]:
            nc.wait_recv()
            nx_out[...] = (
                nv[:, theirs].astype(F32) + nc_in[:, theirs_in].astype(F32)
            ).astype(BF16)
            nx = send(nx_out, nx_in, nx_s.at[0], nx_r.at[0], inst=across)

    def chip_sum(k):
        return (
            gv[k, :, mine].astype(F32)
            + core_in[k, :, mine_in].astype(F32)
            + x_in[k].astype(F32)
        )

    z_c = {}
    ny_c, nz_c = [], []
    for j in order[:-1]:
        x_c[j].wait_recv()
        k = to[j]
        z_out[j] = chip_sum(k).astype(BF16)
        z_c[j] = send(z_out.at[j], z_in.at[j], z_s.at[j], z_r.at[j], dp=k)
        if j == order[0]:
            nx.wait_recv()
            ny[y] = (
                nv[:, mine].astype(F32) + nc_in[:, mine_in].astype(F32)
                + nx_in[...].astype(F32)
            ).astype(BF16)
            for i in range(1, tp):
                ny_c.append(
                    send(ny.at[y], ny.at[y], ny_s.at[i], ny_r.at[i], tp=(y + i) % tp)
                )
    for copy in ny_c:
        copy.wait_recv()
    total = ny[0].astype(F32)
    for i in range(1, tp):
        total += ny[i].astype(F32)
    nz[z] = total.astype(BF16)
    for j in range(1, n):
        nz_c.append(send(nz.at[z], nz.at[z], nz_s.at[j], nz_r.at[j], dp=to[j]))

    x_c[0].wait_recv()
    gradient = chip_sum(z)
    for copy in load_state:
        copy.wait()
    for j in order[:-1]:
        z_c[j].wait_recv()
        gradient += z_in[j].astype(F32)
    gsum[:, mine] = gradient.astype(BF16)

    def new_params(where):
        g = gsum[:, where].astype(F32)
        fresh = adam_update(g, pv[:, where], mv[:, where], vv[:, where])[0]
        params[z, :, where] = fresh.astype(BF16)

    new_params(mine)
    pz_c = {}
    for j in near[::-1]:
        pz_c[j] = send(
            params.at[z, :, mine], params.at[z, :, mine], pz_s.at[j], pz_r.at[j], dp=to[j]
        )
    g_x = send(gsum.at[:, mine], gsum.at[:, mine], g_s.at[0], g_r.at[0], inst=across)
    g_c = send(gsum.at[:, mine], gsum.at[:, mine], g_s.at[1], g_r.at[1], inst=partner)

    for copy in nz_c:
        copy.wait_recv()
    total = nz[0].astype(F32)
    for j in range(1, n):
        total += nz[j].astype(F32)
    gain_sum[:, mine] = total
    nf_c = [
        send(gain_sum.at[:, mine], gain_sum.at[:, mine], nf_s.at[i], nf_r.at[i], inst=other)
        for i, other in enumerate((partner, across, diagonal))
    ]

    g_x.wait_recv()
    g_f = send(gsum.at[:, theirs], gsum.at[:, theirs], g_s.at[2], g_r.at[2], inst=partner)
    px_c, pc_c, pd_c = {}, {}, {}

    def relay(j):
        pz_c[j].wait_recv()
        piece = params.at[frm[j], :, mine]
        px_c[j] = send(piece, piece, px_s.at[j], px_r.at[j], inst=across)
        pc_c[j] = send(piece, piece, pc_s.at[j], pc_r.at[j], inst=partner)

    def relay_core(j):
        px_c[j].wait_recv()
        piece = params.at[frm[j], :, theirs]
        pd_c[j] = send(piece, piece, pc_s.at[n + j], pc_r.at[n + j], inst=partner)

    relay(near[0])
    new_params(theirs)
    g_c.wait_recv()
    new_params(cols_of(partner))
    for j in near[1:]:
        relay(j)
    g_f.wait_recv()
    new_params(cols_of(diagonal))
    for j in near:
        relay_core(j)
    for j in near:
        pc_c[j].wait_recv()
        pd_c[j].wait_recv()
    for copy in nf_c:
        copy.wait_recv()
    for group in (core_c, x_c, z_c, pz_c, px_c, pc_c, pd_c):
        for copy in group.values():
            copy.wait_send()
    for copy in (nc, nx, g_x, g_c, g_f, *ny_c, *nz_c, *nf_c):
        copy.wait_send()


def local(
    n, tp,
    kernel_grads,
    kernel_master,
    kernel_first,
    kernel_second,
    gain_grads,
    gain_master,
    gain_first,
    gain_second,
):
    heads, depth, cols = kernel_grads.shape[1:]
    rows = depth // n
    norms = gain_grads.shape[1]
    half, quarter = cols // 2, cols // 4
    dma = pltpu.SemaphoreType.DMA
    vmem = pl.BlockSpec(memory_space=pltpu.VMEM)
    anyspace = pl.BlockSpec(memory_space=pl.ANY)
    params, gradient, gain_whole = pl.pallas_call(
        functools.partial(step_kernel, n, tp),
        out_shape=(
            jax.ShapeDtypeStruct((n, rows, cols), BF16),
            jax.ShapeDtypeStruct((rows, cols), BF16),
            jax.ShapeDtypeStruct((norms, cols), F32),
        ),
        in_specs=[anyspace] * 5,
        out_specs=(vmem, vmem, vmem),
        scratch_shapes=[
            pltpu.VMEM((n, rows, cols), BF16),
            pltpu.VMEM((n, rows, half), BF16),
            pltpu.VMEM((n, rows, quarter), BF16),
            pltpu.VMEM((n, rows, quarter), BF16),
            pltpu.VMEM((n, rows, quarter), BF16),
            pltpu.VMEM((n, rows, quarter), BF16),
            pltpu.VMEM((rows, cols), F32),
            pltpu.VMEM((rows, cols), F32),
            pltpu.VMEM((rows, cols), F32),
            pltpu.VMEM((norms, cols), BF16),
            pltpu.VMEM((norms, half), BF16),
            pltpu.VMEM((norms, quarter), BF16),
            pltpu.VMEM((norms, quarter), BF16),
            pltpu.VMEM((tp, norms, quarter), BF16),
            pltpu.VMEM((n, norms, quarter), BF16),
            dma((n + 4,)),
            dma((n,)), dma((n,)), dma((n,)), dma((n,)), dma((n,)), dma((n,)),
            dma((n,)), dma((n,)), dma((n,)), dma((n,)), dma((2 * n,)), dma((2 * n,)),
            dma((3,)), dma((3,)),
            dma((1,)), dma((1,)), dma((1,)), dma((1,)),
            dma((tp,)), dma((tp,)), dma((n,)), dma((n,)), dma((3,)), dma((3,)),
        ],
        compiler_params=pltpu.CompilerParams(collective_id=0, has_side_effects=True),
    )(
        kernel_grads.reshape(n, rows, cols),
        kernel_master.reshape(rows, cols),
        kernel_first.reshape(rows, cols),
        kernel_second.reshape(rows, cols),
        gain_grads.reshape(norms, cols),
    )
    kernel_params = params.reshape(heads, depth, cols)
    kernel_master_new, kernel_first_new, kernel_second_new = adam_update(
        gradient.astype(F32).reshape(kernel_master.shape),
        kernel_master, kernel_first, kernel_second,
    )
    gain_master_new, gain_first_new, gain_second_new = adam_update(
        gain_whole, gain_master, gain_first, gain_second
    )
    gain_params = gain_master_new.astype(BF16)
    return (
        kernel_params,
        kernel_master_new,
        kernel_first_new,
        kernel_second_new,
        gain_params,
        gain_master_new,
        gain_first_new,
        gain_second_new,
    )


def solution(mesh):
    return jax.shard_map(
        functools.partial(local, mesh.shape["dp"], mesh.shape["tp"]),
        mesh=mesh,
        in_specs=(
            P(("inst", "dp"), "tp", None, None),
            P("tp", "dp", None),
            P("tp", "dp", None),
            P("tp", "dp", None),
            P(("inst", "dp", "tp"), None, None),
            P(),
            P(),
            P(),
        ),
        out_specs=(
            P("tp", None, None),
            P("tp", "dp", None),
            P("tp", "dp", None),
            P("tp", "dp", None),
            P(),
            P(),
            P(),
            P(),
        ),
        check_vma=False,
    )
```

```python
import functools

import jax
import jax.numpy as jnp
from jax import lax
from jax.experimental import pallas as pl
from jax.experimental.pallas import tpu as pltpu
from jax.sharding import PartitionSpec as P

beta_one = 0.9
beta_two = 0.95
learn_rate = 0.01
decay_rate = 0.1
epsilon = 1e-08
step_count = 100.0
MESH = pl.DeviceIdType.MESH
F32 = jnp.float32
BF16 = jnp.bfloat16


def adam_update(gradient, master, first_moment, second_moment):
    first_next = beta_one * first_moment + (1.0 - beta_one) * gradient
    second_next = beta_two * second_moment + (1.0 - beta_two) * gradient * gradient
    first_hat = first_next / (1.0 - beta_one**step_count)
    second_hat = second_next / (1.0 - beta_two**step_count)
    master_next = master - learn_rate * (
        first_hat / (jnp.sqrt(second_hat) + epsilon) + decay_rate * master
    )
    return (master_next, first_next, second_next)


def step_kernel(
    n, tp, grads, master, first, second, gains,
    params, gsum, gain_sum,
    gv, core_in, x_out, x_in, z_out, z_in, pv, mv, vv,
    nv, nc_in, nx_out, nx_in, ny, nz,
    load_sem, core_s, core_r, x_s, x_r, z_s, z_r,
    pz_s, pz_r, px_s, px_r, pc_s, pc_r, g_s, g_r,
    nc_s, nc_r, nx_s, nx_r, ny_s, ny_r, nz_s, nz_r, nf_s, nf_r,
):
    cols = gv.shape[2]
    half, quarter = cols // 2, cols // 4
    me = lax.axis_index("inst")
    z = lax.axis_index("dp")
    y = lax.axis_index("tp")
    core, x = me % 2, me // 2
    partner = me + 1 - 2 * core
    across = (me + 2) % 4
    diagonal = (partner + 2) % 4
    rows = gv.shape[1]
    parts = 2 if rows % 32 == 0 else 1
    cut = rows // parts

    def ranked(r):
        low = jnp.minimum(z, n - 1 - z)
        both = r <= 2 * low
        dist = jnp.where(both, (r + 1) // 2, r - low)
        up = jnp.where(both, 1 - r % 2, (2 * z < n - 1).astype(jnp.int32))
        return z + (2 * up - 1) * dist

    ring = {0: z, **{r: ranked(r) for r in range(1, n)}}
    order = list(range(n - 1, -1, -1))
    near = list(range(1, n))
    pieces = [(r, p) for r in order for p in range(parts)]

    def band(p):
        return pl.ds(p * cut, cut)

    def span(start, size):
        return pl.ds(pl.multiple_of(start, 128), size)

    def cols_of(inst):
        return span((inst % 2) * half + (inst // 2) * quarter, quarter)

    def send(src, dst, s, r, **where):
        copy = pltpu.make_async_remote_copy(
            src_ref=src, dst_ref=dst, send_sem=s, recv_sem=r,
            device_id=where, device_id_type=MESH,
        )
        copy.start()
        return copy

    def load(src, dst, k):
        copy = pltpu.make_async_copy(src, dst, load_sem.at[k])
        copy.start()
        return copy

    loads = {j: load(grads.at[ring[j]], gv.at[ring[j]], j) for j in order}
    load_gain = load(gains, nv, n)
    load_state = [
        load(a, b, n + 1 + k)
        for k, (a, b) in enumerate(((master, pv), (first, mv), (second, vv)))
    ]

    barrier = pltpu.get_barrier_semaphore()
    for other in (partner, across, diagonal):
        pl.semaphore_signal(barrier, inc=1, device_id={"inst": other}, device_id_type=MESH)
    for j in range(1, n):
        pl.semaphore_signal(barrier, inc=1, device_id={"dp": ring[j]}, device_id_type=MESH)
    for j in range(1, tp):
        pl.semaphore_signal(
            barrier, inc=1, device_id={"tp": (y + j) % tp}, device_id_type=MESH
        )
    pl.semaphore_wait(barrier, 3 + n - 1 + tp - 1)

    mine_half, other_half = span(core * half, half), span((1 - core) * half, half)
    mine, theirs = cols_of(me), cols_of(across)
    mine_in, theirs_in = span(x * quarter, quarter), span((1 - x) * quarter, quarter)
    sent = []

    core_c = {}
    for r, p in pieces:
        if p == 0:
            loads[r].wait()
        k = ring[r]
        core_c[r, p] = send(
            gv.at[k, band(p), other_half], core_in.at[k, band(p)],
            core_s.at[r, p], core_r.at[r, p], inst=partner,
        )
    load_gain.wait()
    nc = send(nv.at[:, other_half], nc_in, nc_s.at[0], nc_r.at[0], inst=partner)

    x_c = {}
    for r, p in pieces:
        core_c[r, p].wait_recv()
        k, rows_p = ring[r], band(p)
        x_out[k, rows_p] = (
            gv[k, rows_p, theirs].astype(F32) + core_in[k, rows_p, theirs_in].astype(F32)
        ).astype(BF16)
        x_c[r, p] = send(
            x_out.at[k, rows_p], x_in.at[k, rows_p], x_s.at[r, p], x_r.at[r, p], inst=across
        )
        if (r, p) == pieces[1]:
            nc.wait_recv()
            nx_out[...] = (
                nv[:, theirs].astype(F32) + nc_in[:, theirs_in].astype(F32)
            ).astype(BF16)
            nx = send(nx_out, nx_in, nx_s.at[0], nx_r.at[0], inst=across)

    def chip_sum(k, rows_p):
        return (
            gv[k, rows_p, mine].astype(F32)
            + core_in[k, rows_p, mine_in].astype(F32)
            + x_in[k, rows_p].astype(F32)
        )

    z_c = {}
    ny_c, nz_c = [], []
    for r, p in pieces[: -parts]:
        x_c[r, p].wait_recv()
        k, rows_p = ring[r], band(p)
        z_out[k, rows_p] = chip_sum(k, rows_p).astype(BF16)
        z_c[r, p] = send(
            z_out.at[k, rows_p], z_in.at[z, rows_p], z_s.at[r, p], z_r.at[z, p], dp=k
        )
        if (r, p) == pieces[1]:
            nx.wait_recv()
            ny[y] = (
                nv[:, mine].astype(F32) + nc_in[:, mine_in].astype(F32)
                + nx_in[...].astype(F32)
            ).astype(BF16)
            for i in range(1, tp):
                ny_c.append(
                    send(ny.at[y], ny.at[y], ny_s.at[i], ny_r.at[i], tp=(y + i) % tp)
                )
    for copy in ny_c:
        copy.wait_recv()
    total = ny[0].astype(F32)
    for i in range(1, tp):
        total += ny[i].astype(F32)
    nz[z] = total.astype(BF16)
    for j in near:
        nz_c.append(
            send(nz.at[z], nz.at[z], nz_s.at[j], nz_r.at[j], dp=(z + j) % n)
        )

    def expect(ref, s, r, **where):
        return pltpu.make_async_remote_copy(
            src_ref=ref, dst_ref=ref, send_sem=s, recv_sem=r,
            device_id=where, device_id_type=MESH,
        )

    for copy in load_state:
        copy.wait()

    def new_params(where, rows_p):
        g = gsum[rows_p, where].astype(F32)
        fresh = adam_update(g, pv[rows_p, where], mv[rows_p, where], vv[rows_p, where])[0]
        params[z, rows_p, where] = fresh.astype(BF16)

    pz_c, g_x, g_c, g_f = {}, {}, {}, {}
    for p in range(parts):
        rows_p = band(p)
        x_c[0, p].wait_recv()
        gradient = chip_sum(z, rows_p)
        for r in near:
            k = ring[r]
            expect(z_in.at[k, rows_p], z_s.at[r, p], z_r.at[k, p], dp=k).wait_recv()
            gradient += z_in[k, rows_p].astype(F32)
        gsum[rows_p, mine] = gradient.astype(BF16)
        new_params(mine, rows_p)
        piece = params.at[z, rows_p, mine]
        for r in near:
            pz_c[r, p] = send(piece, piece, pz_s.at[r, p], pz_r.at[z, p], dp=ring[r])
        piece = gsum.at[rows_p, mine]
        g_x[p] = send(piece, piece, g_s.at[0, p], g_r.at[0, p], inst=across)
        g_c[p] = send(piece, piece, g_s.at[1, p], g_r.at[1, p], inst=partner)

    for copy in nz_c:
        copy.wait_recv()
    total = nz[0].astype(F32)
    for j in range(1, n):
        total += nz[j].astype(F32)
    gain_sum[:, mine] = total
    nf_c = [
        send(gain_sum.at[:, mine], gain_sum.at[:, mine], nf_s.at[i], nf_r.at[i], inst=other)
        for i, other in enumerate((partner, across, diagonal))
    ]

    px_c, pc_c, pd_c = {}, {}, {}

    def relay(r):
        for p in range(parts):
            k = ring[r]
            piece = params.at[k, band(p), mine]
            expect(piece, pz_s.at[r, p], pz_r.at[k, p], dp=k).wait_recv()
            px_c[r, p] = send(piece, piece, px_s.at[r, p], px_r.at[r, p], inst=across)
            pc_c[r, p] = send(piece, piece, pc_s.at[r, p], pc_r.at[r, p], inst=partner)

    def relay_core(r):
        for p in range(parts):
            px_c[r, p].wait_recv()
            piece = params.at[ring[r], band(p), theirs]
            pd_c[r, p] = send(
                piece, piece, pc_s.at[n + r, p], pc_r.at[n + r, p], inst=partner
            )

    relay(near[0])
    for p in range(parts):
        g_x[p].wait_recv()
        piece = gsum.at[band(p), theirs]
        g_f[p] = send(piece, piece, g_s.at[2, p], g_r.at[2, p], inst=partner)
    for r in near[1:-1]:
        relay(r)
    for p in range(parts):
        g_c[p].wait_recv()
        new_params(theirs, band(p))
        new_params(cols_of(partner), band(p))
    for r in near[1:][-1:]:
        relay(r)
    for p in range(parts):
        g_f[p].wait_recv()
        new_params(cols_of(diagonal), band(p))
    for r in near:
        relay_core(r)
    for key in pc_c:
        pc_c[key].wait_recv()
        pd_c[key].wait_recv()
    for copy in nf_c:
        copy.wait_recv()
    for group in (core_c, x_c, z_c, pz_c, px_c, pc_c, pd_c, g_x, g_c, g_f):
        for copy in group.values():
            copy.wait_send()
    for copy in (nc, nx, *ny_c, *nz_c, *nf_c):
        copy.wait_send()


def local(
    n, tp,
    kernel_grads,
    kernel_master,
    kernel_first,
    kernel_second,
    gain_grads,
    gain_master,
    gain_first,
    gain_second,
):
    heads, depth, cols = kernel_grads.shape[1:]
    rows = depth // n
    norms = gain_grads.shape[1]
    half, quarter = cols // 2, cols // 4
    parts = 2
    dma = pltpu.SemaphoreType.DMA
    vmem = pl.BlockSpec(memory_space=pltpu.VMEM)
    hbm = pl.BlockSpec(memory_space=pltpu.HBM)
    params, gradient, gain_whole = pl.pallas_call(
        functools.partial(step_kernel, n, tp),
        out_shape=(
            jax.ShapeDtypeStruct((n, rows, cols), BF16),
            jax.ShapeDtypeStruct((rows, cols), BF16),
            jax.ShapeDtypeStruct((norms, cols), F32),
        ),
        in_specs=[hbm] * 5,
        out_specs=(vmem, vmem, vmem),
        scratch_shapes=[
            pltpu.VMEM((n, rows, cols), BF16),
            pltpu.VMEM((n, rows, half), BF16),
            pltpu.VMEM((n, rows, quarter), BF16),
            pltpu.VMEM((n, rows, quarter), BF16),
            pltpu.VMEM((n, rows, quarter), BF16),
            pltpu.VMEM((n, rows, quarter), BF16),
            pltpu.VMEM((rows, cols), F32),
            pltpu.VMEM((rows, cols), F32),
            pltpu.VMEM((rows, cols), F32),
            pltpu.VMEM((norms, cols), BF16),
            pltpu.VMEM((norms, half), BF16),
            pltpu.VMEM((norms, quarter), BF16),
            pltpu.VMEM((norms, quarter), BF16),
            pltpu.VMEM((tp, norms, quarter), BF16),
            pltpu.VMEM((n, norms, quarter), BF16),
            dma((n + 4,)),
            *[dma((n, parts))] * 10,
            dma((2 * n, parts)), dma((2 * n, parts)), dma((3, parts)), dma((3, parts)),
            dma((1,)), dma((1,)), dma((1,)), dma((1,)),
            dma((tp,)), dma((tp,)), dma((n,)), dma((n,)), dma((3,)), dma((3,)),
        ],
        compiler_params=pltpu.CompilerParams(collective_id=0, has_side_effects=True, vmem_limit_bytes=16 * 2**20),
    )(
        *(
            pltpu.with_memory_space_constraint(array, pltpu.HBM)
            for array in (
                kernel_grads.reshape(n, rows, cols),
                kernel_master.reshape(rows, cols),
                kernel_first.reshape(rows, cols),
                kernel_second.reshape(rows, cols),
                gain_grads.reshape(norms, cols),
            )
        )
    )
    kernel_params = params.reshape(heads, depth, cols)
    kernel_master_new, kernel_first_new, kernel_second_new = adam_update(
        gradient.astype(F32).reshape(kernel_master.shape),
        kernel_master, kernel_first, kernel_second,
    )
    gain_master_new, gain_first_new, gain_second_new = adam_update(
        gain_whole, gain_master, gain_first, gain_second
    )
    gain_params = gain_master_new.astype(BF16)
    return (
        kernel_params,
        kernel_master_new,
        kernel_first_new,
        kernel_second_new,
        gain_params,
        gain_master_new,
        gain_first_new,
        gain_second_new,
    )


def solution(mesh):
    return jax.shard_map(
        functools.partial(local, mesh.shape["dp"], mesh.shape["tp"]),
        mesh=mesh,
        in_specs=(
            P(("inst", "dp"), "tp", None, None),
            P("tp", "dp", None),
            P("tp", "dp", None),
            P("tp", "dp", None),
            P(("inst", "dp", "tp"), None, None),
            P(),
            P(),
            P(),
        ),
        out_specs=(
            P("tp", None, None),
            P("tp", "dp", None),
            P("tp", "dp", None),
            P("tp", "dp", None),
            P(),
            P(),
            P(),
            P(),
        ),
        check_vma=False,
    )
```
